32 devices in a mesh: batch: 8 (over z, x), seq: 4 (over y, core).
Axes of the slice: x: 2, y: 2, z: 4, core: 2. Of those that a mesh axis runs over, the one named last changes fastest.
Arguments:
- hidden_in: bfloat16 [8, 512, 2048], P('batch', 'seq'), may hold values from -6 to 6
- queries: bfloat16 [8, 512, 2048], P('batch', 'seq'), may hold values from -5 to 5
- key_states: bfloat16 [8, 512, 512], P('batch', 'seq'), may hold values from -12 to 12
- value_states: bfloat16 [8, 512, 512], P('batch', 'seq'), may hold values from -6 to 6
- grad_out: bfloat16 [8, 512, 2048], P('batch', 'seq'), may hold values from -6 to 6
- log_sums: float32 [8, 16, 512], P('batch', None, 'seq'), may hold values from -700 to 700, as said below
- deltas: float32 [8, 16, 512], P('batch', None, 'seq'), may hold values from -6 to 6
- block_order: int32 [8], replicated, may hold values from 0 to 7, as said below
Outputs:
- grad_queries: bfloat16 [8, 512, 2048], P('batch', 'seq')
- grad_keys: bfloat16 [8, 512, 512], P('batch', 'seq')
- grad_values: bfloat16 [8, 512, 512], P('batch', 'seq')
- key_wgrad: float32 [2048, 512], P(('batch', 'seq'))
- value_wgrad: float32 [2048, 512], P(('batch', 'seq'))
The draws below stay inside these ranges and needn't reach their ends.
Inputs may be any that keep to these rules, and one draw needn't show every extreme that they name: `block_order`: entries 2i and 2i+1 name blocks c and 7 - c for some c, in either order; the 8 entries together are a permutation of 0 to 7. `log_sums`: each entry lies within 0.1 of the log of the sum over visible j of exp(scores[b,h,i,j]).
All inputs are finite; a program needn't handle non-finite values.
Results may differ from the reference program's by a relative error of at most 0.0049.
Values may be sent and summed in bfloat16 or wider, within the bound.
No kernel may reach another device: no remote copies, remote signals or barrier semaphores. Data moves between devices by JAX's collectives and lax.ppermute only.
A program may use at most 64 MiB of HBM per device.

```python
import math
import jax
import jax.numpy as jnp
from jax import lax

HQ = 16
HK = 4
DH = 128
DIN = 2048
SEQ = 512
BATCH = 8
BLOCK = 64
BLOCKS = 8
GROUP = 4
QW = 2048
KW = 512


def draw_queries(key, part):
    normal_part = jnp.clip(jax.random.normal(jax.random.fold_in(key, 11), (BATCH, SEQ, HQ * DH), jnp.float32), -4.0, 4.0)
    return normal_part.astype(jnp.bfloat16)


def draw_key_states(key, part):
    normal_part = jnp.clip(jax.random.normal(jax.random.fold_in(key, 13), (BATCH, SEQ, HK * DH), jnp.float32), -4.0, 4.0)
    return normal_part.astype(jnp.bfloat16)


def draw_block_order(key, part):
    pair_key, flip_key = jax.random.split(jax.random.fold_in(key, 29))
    pair_ids = jax.random.permutation(pair_key, BLOCKS // 2).astype(jnp.int32)
    flip_bits = jax.random.randint(flip_key, (BLOCKS // 2,), 0, 2)
    first_block = jnp.where(flip_bits == 1, BLOCKS - 1 - pair_ids, pair_ids)
    second_block = BLOCKS - 1 - first_block
    return jnp.stack([first_block, second_block], axis=1).reshape(BLOCKS).astype(jnp.int32)


def draw_log_sums(key, part):
    query_all = draw_queries(key, part).astype(jnp.float32)
    key_all = draw_key_states(key, part).astype(jnp.float32)
    order = draw_block_order(key, part)
    row_ids = jnp.arange(SEQ, dtype=jnp.int32)
    position = order[row_ids // BLOCK] * BLOCK + row_ids % BLOCK
    visible = position[None, :] <= position[:, None]

    def one_group(group_ops):
        group_queries, group_keys = group_ops
        scores = jnp.einsum('igd,jd->gij', group_queries, group_keys) * (1.0 / math.sqrt(DH))
        scores = jnp.where(visible[None, :, :], scores, -jnp.inf)
        return jax.nn.logsumexp(scores, axis=-1)

    def one_sequence(seq_ops):
        seq_queries, seq_keys = seq_ops
        queries_head = jnp.moveaxis(seq_queries.reshape(SEQ, HK, GROUP, DH), 1, 0)
        keys_head = jnp.moveaxis(seq_keys.reshape(SEQ, HK, DH), 1, 0)
        return lax.map(one_group, (queries_head, keys_head)).reshape(HQ, SEQ)
    exact = lax.map(one_sequence, (query_all, key_all))
    noise = jax.random.uniform(jax.random.fold_in(key, 41), (BATCH, HQ, SEQ), jnp.float32, -0.1, 0.1)
    return (exact + noise).astype(jnp.float32)


def spiked(result, stream_key, source, target, blocks, factor):
    def block_of(dim):
        return (jnp.arange(result.shape[dim]) // (result.shape[dim] // blocks)).reshape((-1,) + (1,) * (result.ndim - 1 - dim))

    one_side = jax.random.permutation(stream_key, blocks)[block_of(target)]
    far = (block_of(target) + blocks // 2) % blocks
    return jnp.where((block_of(source) == one_side) | (block_of(source) == far), factor * result, result)


def block_scale(rng, shape, cuts, smallest, top_value):
    def one(dim, blocks):
        steps = jax.random.uniform(jax.random.fold_in(jax.random.fold_in(rng, 6), dim), (blocks,), jnp.float32, smallest / len(cuts), top_value / len(cuts))
        return jnp.repeat(jnp.exp(steps), shape[dim] // blocks).reshape((-1,) + (1,) * (len(shape) - dim - 1))

    factor_of = one(*cuts[0])
    for cut in cuts[1:]:
        factor_of = factor_of * one(*cut)
    return factor_of


def scatter_about(rng, dims, width, reach, cuts=(), kind=jnp.bfloat16):
    loudness = block_scale(rng, dims, cuts, -0.22, 0.18) if cuts else 1.0
    entries = jax.random.normal(rng, dims, jnp.float32) * width * loudness
    return jnp.minimum(jnp.maximum(entries, -reach), reach).astype(kind)


def heavy_noise(rng, dims, width, reach, cuts, heavy, held_as=jnp.bfloat16):
    result = width * jax.random.normal(rng, dims, jnp.float32)
    if cuts:
        result = result * block_scale(rng, dims, cuts, -0.22, 0.18)
    return jnp.clip(spiked(result, jax.random.fold_in(rng, 3), *heavy), -reach, reach).astype(held_as)


def setup_inputs(seed: int = 0) -> dict:
    arg_keys = jax.random.split(jax.random.key(seed), 9)
    hidden_in = heavy_noise(arg_keys[0], (BATCH, SEQ, DIN), 1.0, 6.0, ((0, 8), (1, 4)), (1, 2, 4, 2.0))
    queries = draw_queries(jax.random.fold_in(arg_keys[8], 71), 0)
    key_states = draw_key_states(jax.random.fold_in(arg_keys[8], 71), 0)
    value_states = scatter_about(arg_keys[3], (BATCH, SEQ, KW), 1.0, 6.0, ((0, 8), (1, 4)))
    grad_out = scatter_about(arg_keys[4], (BATCH, SEQ, QW), 1.0, 6.0, ((0, 8), (1, 4)))
    log_sums = draw_log_sums(jax.random.fold_in(arg_keys[8], 71), 0)
    deltas = scatter_about(arg_keys[6], (BATCH, HQ, SEQ), 1.0, 6.0, ((0, 8), (2, 4)), jnp.float32)
    block_order = draw_block_order(jax.random.fold_in(arg_keys[8], 71), 0)
    return {"hidden_in": hidden_in, "queries": queries, "key_states": key_states, "value_states": value_states, "grad_out": grad_out, "log_sums": log_sums, "deltas": deltas, "block_order": block_order}


def group_grads(operands, position):
    group_queries, group_keys, group_values, group_cots, group_lse, group_deltas = operands
    scale_factor = 1.0 / math.sqrt(DH)
    query_full = group_queries.astype(jnp.float32)
    key_full = group_keys.astype(jnp.float32)
    value_full = group_values.astype(jnp.float32)
    grad_full = group_cots.astype(jnp.float32)
    scores = jnp.einsum('igd,jd->gij', query_full, key_full) * scale_factor
    visible = position[None, :] <= position[:, None]
    scores = jnp.where(visible[None, :, :], scores, -jnp.inf)
    probs = jnp.exp(scores - group_lse[..., None])
    grad_probs = jnp.einsum('igd,jd->gij', grad_full, value_full)
    grad_scores = (probs * (grad_probs - group_deltas[..., None]) * scale_factor).astype(jnp.bfloat16)
    grad_scores = lax.optimization_barrier(grad_scores).astype(jnp.float32)
    probs_low = lax.optimization_barrier(probs.astype(jnp.bfloat16)).astype(jnp.float32)
    query_grad = jnp.einsum('gij,jd->igd', grad_scores, key_full)
    key_grad = jnp.einsum('gij,igd->jd', grad_scores, query_full)
    value_grad = jnp.einsum('gij,igd->jd', probs_low, grad_full)
    return (query_grad, key_grad, value_grad)

def sequence_grads(operands, position):
    seq_queries, seq_keys, seq_values, seq_cots, seq_lse, seq_deltas = operands
    group_size = HQ // HK
    queries_head = jnp.moveaxis(seq_queries.reshape(SEQ, HK, group_size, DH), 1, 0)
    keys_head = jnp.moveaxis(seq_keys.reshape(SEQ, HK, DH), 1, 0)
    values_head = jnp.moveaxis(seq_values.reshape(SEQ, HK, DH), 1, 0)
    cots_head = jnp.moveaxis(seq_cots.reshape(SEQ, HK, group_size, DH), 1, 0)
    lse_head = seq_lse.reshape(HK, group_size, SEQ)
    deltas_head = seq_deltas.reshape(HK, group_size, SEQ)
    query_grad, key_grad, value_grad = lax.map(lambda group_ops: group_grads(group_ops, position), (queries_head, keys_head, values_head, cots_head, lse_head, deltas_head))
    query_grad = jnp.moveaxis(query_grad, 0, 1).reshape(SEQ, HQ * DH)
    key_grad = jnp.moveaxis(key_grad, 0, 1).reshape(SEQ, HK * DH)
    value_grad = jnp.moveaxis(value_grad, 0, 1).reshape(SEQ, HK * DH)
    return (query_grad.astype(jnp.bfloat16), key_grad.astype(jnp.bfloat16), value_grad.astype(jnp.bfloat16))

def reference(hidden_in, queries, key_states, value_states, grad_out, log_sums, deltas, block_order):
    row_ids = jnp.arange(SEQ, dtype=jnp.int32)
    position = (block_order[row_ids // BLOCK] * BLOCK + row_ids % BLOCK).astype(jnp.int32)
    grad_queries, grad_keys, grad_values = lax.map(lambda seq_ops: sequence_grads(seq_ops, position), (queries, key_states, value_states, grad_out, log_sums, deltas))
    flat_hidden = hidden_in.reshape(BATCH * SEQ, DIN)
    key_wgrad = jnp.dot(flat_hidden.T, grad_keys.reshape(BATCH * SEQ, HK * DH), preferred_element_type=jnp.float32)
    value_wgrad = jnp.dot(flat_hidden.T, grad_values.reshape(BATCH * SEQ, HK * DH), preferred_element_type=jnp.float32)
    return (grad_queries, grad_keys, grad_values, key_wgrad, value_wgrad)
```

```python
import math

import jax
import jax.numpy as jnp
from jax import lax
from jax.experimental import pallas as pl
from jax.experimental.pallas import tpu as pltpu
from jax.sharding import PartitionSpec as P

HQ = 16
HK = 4
DH = 128


MASKED = -1e30


def passed_along(value, axis, steps):
    count = lax.axis_size(axis)
    pairs = [(source, (source + steps) % count) for source in range(count)]
    return lax.ppermute(value, axis, pairs)


def stored_positions(block_order, first_row, row_count, span_rows):
    row_ids = first_row + jnp.arange(row_count, dtype=jnp.int32)
    slot_ids = row_ids // span_rows
    matches = slot_ids[:, None] == jnp.arange(block_order.shape[0], dtype=jnp.int32)[None, :]
    block_ids = jnp.sum(jnp.where(matches, block_order[None, :], 0), axis=1)
    return block_ids * span_rows + row_ids % span_rows


def head_scores(left_heads, right_block):
    batch_rows, right_rows = (right_block.shape[0], right_block.shape[1])
    right_heads = right_block.reshape(batch_rows, right_rows, HK, DH)
    return jnp.einsum(
        "bqhgd,bkhd->bhgqk", left_heads, right_heads, preferred_element_type=jnp.float32
    )


def masked_scores(query_heads, key_block, query_pos, key_pos):
    scores = head_scores(query_heads, key_block) * (1.0 / math.sqrt(DH))
    visible = key_pos[None, :] <= query_pos[:, None]
    return jnp.where(visible, scores, MASKED)


def grad_block(
    query_heads, grad_heads, query_pos, row_lse, row_deltas, key_block, value_block, key_pos
):
    scores = masked_scores(query_heads, key_block, query_pos, key_pos)
    probs = jnp.exp(scores - row_lse[..., None])
    grad_probs = head_scores(grad_heads, value_block)
    grad_scores = (probs * (grad_probs - row_deltas[..., None]) * (1.0 / math.sqrt(DH))).astype(
        jnp.bfloat16
    )
    probs_low = probs.astype(jnp.bfloat16)
    batch_rows, key_rows = (key_block.shape[0], key_block.shape[1])
    key_heads = key_block.reshape(batch_rows, key_rows, HK, DH)
    query_part = jnp.einsum(
        "bhgqk,bkhd->bqhgd", grad_scores, key_heads, preferred_element_type=jnp.float32
    )
    key_part = jnp.einsum(
        "bhgqk,bqhgd->bkhd", grad_scores, query_heads, preferred_element_type=jnp.float32
    )
    value_part = jnp.einsum(
        "bhgqk,bqhgd->bkhd", probs_low, grad_heads, preferred_element_type=jnp.float32
    )
    key_part = key_part.reshape(batch_rows, key_rows, HK * DH)
    value_part = value_part.reshape(batch_rows, key_rows, HK * DH)
    return (query_part, key_part, value_part)


def ring_shards(hidden_in, queries, key_states, value_states, grad_out, log_sums, deltas, block_order):
    seq_count = lax.axis_size("seq")
    my_index = lax.axis_index("seq")
    batch_rows, local_rows = (queries.shape[0], queries.shape[1])
    span_rows = local_rows // 2
    group_size = HQ // HK
    query_heads = queries.reshape(batch_rows, local_rows, HK, group_size, DH)
    grad_heads = grad_out.reshape(batch_rows, local_rows, HK, group_size, DH)
    row_lse = log_sums.reshape(batch_rows, HK, group_size, local_rows)
    row_deltas = deltas.reshape(batch_rows, HK, group_size, local_rows)
    query_pos = stored_positions(block_order, my_index * local_rows, local_rows, span_rows)
    key_zeros = jnp.zeros(key_states.shape, jnp.float32)
    query_zeros = jnp.zeros(query_heads.shape, jnp.float32)

    def block_grads(accums, key_block, value_block, source):
        key_acc, value_acc, query_acc = accums
        key_pos = stored_positions(block_order, source * local_rows, local_rows, span_rows)
        query_part, key_part, value_part = grad_block(
            query_heads, grad_heads, query_pos, row_lse, row_deltas, key_block, value_block, key_pos
        )
        return (key_acc + key_part, value_acc + value_part, query_acc + query_part)

    whole_keys, whole_values = (
        lax.all_gather(key_states, "seq", axis=1, tiled=True),
        lax.all_gather(value_states, "seq", axis=1, tiled=True),
    )

    def back_turn(turn_index, accums):
        source = (my_index + turn_index + 1) % seq_count
        key_block = lax.dynamic_slice_in_dim(whole_keys, source * local_rows, local_rows, 1)
        value_block = lax.dynamic_slice_in_dim(whole_values, source * local_rows, local_rows, 1)
        return block_grads(accums, key_block, value_block, source)

    def back_step(turn_index, accums):
        key_acc, value_acc, query_acc = back_turn(turn_index, accums)
        key_acc, value_acc = passed_along((key_acc, value_acc), "seq", -1)
        return (key_acc, value_acc, query_acc)

    accums = lax.fori_loop(0, seq_count - 1, back_step, (key_zeros, key_zeros, query_zeros))
    key_acc, value_acc, query_acc = back_turn(seq_count - 1, accums)
    grad_keys = key_acc.astype(jnp.bfloat16)
    grad_values = value_acc.astype(jnp.bfloat16)
    grad_queries = query_acc.reshape(batch_rows, local_rows, HQ * DH).astype(jnp.bfloat16)
    key_width = HK * DH
    token_grads = jnp.concatenate([grad_keys, grad_values], axis=2).reshape(
        batch_rows * local_rows, 2 * key_width
    )
    flat_hidden = hidden_in.reshape(batch_rows * local_rows, hidden_in.shape[2])
    weight_grads = lax.psum_scatter(
        jnp.einsum("td,te->de", flat_hidden, token_grads, preferred_element_type=jnp.float32),
        ("batch", "seq"),
        scatter_dimension=0,
        tiled=True,
    )
    return (
        grad_queries,
        grad_keys,
        grad_values,
        weight_grads[:, :key_width],
        weight_grads[:, key_width:],
    )


def swapped(value, axis, distance):
    count = lax.axis_size(axis)
    return lax.ppermute(value, axis, [(source, source ^ distance) for source in range(count)])


def dot(left, right, left_dim, right_dim):
    dims = (((left_dim,), (right_dim,)), ((), ()))
    return lax.dot_general(left, right, dims, preferred_element_type=jnp.float32)


def vmem():
    return pl.BlockSpec(memory_space=pltpu.VMEM)


def smem():
    return pl.BlockSpec(memory_space=pltpu.SMEM)


def call(body, out_shapes, operands, scalars, scratch=()):
    specs = [smem()] * scalars + [vmem()] * (len(operands) - scalars)
    outs = pl.pallas_call(
        body,
        out_shape=out_shapes,
        in_specs=specs,
        out_specs=[vmem()] * len(out_shapes),
        scratch_shapes=scratch,
        name=body.__name__,
    )(*operands)
    return list(outs)


def shaped(shape, dtype=jnp.bfloat16):
    return jax.ShapeDtypeStruct(shape, dtype)


def head_payloads(place, queries, grad_out, keys, values, count):
    rows, query_width = queries.shape
    key_width = keys.shape[1]
    query_part, key_part = (query_width // count, key_width // count)

    def pack_heads(place_ref, query_ref, grad_ref, key_ref, value_ref, *out_refs):
        for distance, out_ref in enumerate(out_refs):
            peer = place_ref[0] ^ distance
            wide = pl.ds(pl.multiple_of(peer * query_part, query_part), query_part)
            thin = pl.ds(pl.multiple_of(peer * key_part, key_part), key_part)
            out_ref[:, :query_part] = query_ref[:, wide]
            out_ref[:, query_part : 2 * query_part] = grad_ref[:, wide]
            out_ref[:, 2 * query_part : 2 * query_part + key_part] = key_ref[:, thin]
            out_ref[:, 2 * query_part + key_part :] = value_ref[:, thin]

    shape = shaped((rows, 2 * query_part + 2 * key_part))
    return call(pack_heads, [shape] * count, (place, queries, grad_out, keys, values), 1)


def feature_payloads(place, hidden, count, owners):
    rows, width = hidden.shape
    own = width // (count * owners)

    def pack_features(place_ref, hidden_ref, *refs):
        out_refs, turned_ref = (refs[:-1], refs[-1])
        turned_ref[...] = hidden_ref[...].T
        for distance, out_ref in enumerate(out_refs):
            peer = place_ref[0] ^ distance
            for owner in range(owners):
                first = pl.multiple_of((owner * count + peer) * own, own)
                out_ref[owner * own : (owner + 1) * own, :] = turned_ref[pl.ds(first, own), :]

    shape = shaped((owners * own, rows))
    scratch = [pltpu.VMEM((width, rows), jnp.bfloat16)]
    return call(pack_features, [shape] * count, (place, hidden), 1, scratch)


def head_grads(order, payloads, row_terms, span_rows):
    count = len(payloads)
    rows = payloads[0].shape[0]
    group_size = row_terms[0].shape[0] // 2
    total = count * rows
    spans = total // span_rows
    tile = min(total, 256)
    query_part = group_size * DH

    def attention_grads(order_ref, *refs):
        data_refs, term_refs = (refs[:count], refs[count : 2 * count])
        query_refs, token_ref = (refs[2 * count : 3 * count], refs[3 * count])

        def positions(shape, dim):
            ids = lax.broadcasted_iota(jnp.int32, shape, dim)
            result = ids % span_rows
            slots = ids // span_rows
            for span in range(spans):
                result = jnp.where(slots == span, result + order_ref[span] * span_rows, result)
            return result

        def columns(first):
            return jnp.concatenate([ref[:, first : first + DH] for ref in data_refs], axis=0)

        query_pos = positions((1, total), 1)
        key_pos = positions((total, 1), 0)
        keys = columns(2 * query_part)
        values = columns(2 * query_part + DH)
        scale = 1.0 / math.sqrt(DH)
        hidden_add = [
            jnp.where(key_pos[first : first + tile] <= query_pos, 0.0, MASKED)
            for first in range(0, total, tile)
        ]
        key_sums = [None] * (total // tile)
        value_sums = [None] * (total // tile)
        for head in range(group_size):
            queries = columns(head * DH)
            grads = columns(query_part + head * DH)
            lse = jnp.concatenate([ref[head : head + 1, :] for ref in term_refs], axis=1)
            deltas = jnp.concatenate(
                [ref[group_size + head : group_size + head + 1, :] for ref in term_refs], axis=1
            )
            query_sum = None
            for index in range(total // tile):
                part = slice(index * tile, (index + 1) * tile)
                scores = dot(keys[part], queries, 1, 1) * scale + hidden_add[index]
                probs = jnp.exp(scores - lse)
                grad_probs = dot(values[part], grads, 1, 1)
                grad_scores = (probs * (grad_probs - deltas) * scale).astype(jnp.bfloat16)
                key_part = dot(grad_scores, queries, 1, 0)
                value_part = dot(probs.astype(jnp.bfloat16), grads, 1, 0)
                query_tile = dot(grad_scores, keys[part], 0, 0)
                query_sum = query_tile if index == 0 else query_sum + query_tile
                key_sums[index] = key_part if head == 0 else key_sums[index] + key_part
                value_sums[index] = value_part if head == 0 else value_sums[index] + value_part
            for place, out_ref in enumerate(query_refs):
                out_ref[:, head * DH : (head + 1) * DH] = query_sum[
                    place * rows : (place + 1) * rows
                ].astype(jnp.bfloat16)
        for index in range(total // tile):
            part = slice(index * tile, (index + 1) * tile)
            token_ref[part, :DH] = key_sums[index].astype(jnp.bfloat16)
            token_ref[part, DH:] = value_sums[index].astype(jnp.bfloat16)

    shapes = [shaped((rows, query_part))] * count + [shaped((total, 2 * DH))]
    outs = call(attention_grads, shapes, (order, *payloads, *row_terms), 1)
    return (outs[:count], outs[count])


def weight_parts(places, features, tokens, owners):
    count = len(features)
    width, rows = features[0].shape
    own = width // owners

    def weight_grads(place_ref, owner_ref, *refs):
        feature_refs, token_refs = (refs[:count], refs[count : 2 * count])
        own_ref, key_ref, value_ref = refs[2 * count : 2 * count + 3]
        part_refs, sum_ref = (refs[2 * count + 3 : -1], refs[-1])
        left = jnp.concatenate([ref[...] for ref in feature_refs], axis=1)
        for column, token_ref in enumerate(token_refs):
            right = jnp.concatenate(
                [
                    token_ref[(column ^ source) * rows : ((column ^ source) + 1) * rows, :]
                    for source in range(count)
                ],
                axis=0,
            )
            sum_ref[:, column * 2 * DH : (column + 1) * 2 * DH] = dot(left, right, 1, 0)
            head = pl.multiple_of((place_ref[0] ^ column) * DH, DH)
            mine = slice(column * rows, (column + 1) * rows)
            key_ref[:, pl.ds(head, DH)] = token_ref[mine, :DH]
            value_ref[:, pl.ds(head, DH)] = token_ref[mine, DH:]
        first = pl.multiple_of(owner_ref[0] * own, own)
        own_ref[...] = sum_ref[pl.ds(first, own), :]
        for index, part_ref in enumerate(part_refs):
            first = pl.multiple_of((owner_ref[0] ^ (index + 1)) * own, own)
            part_ref[...] = sum_ref[pl.ds(first, own), :].astype(jnp.bfloat16)

    columns = count * 2 * DH
    shapes = [shaped((own, columns), jnp.float32)] + [shaped((rows, count * DH))] * 2
    shapes += [shaped((own, columns))] * (owners - 1)
    scratch = [pltpu.VMEM((width, columns), jnp.float32)]
    outs = call(weight_grads, shapes, (*places, *features, *tokens), 2, scratch)
    return (outs[0], outs[1], outs[2], outs[3:])


def summed_parts(place, own, parts, count):
    rows = own.shape[0]

    def sum_parts(place_ref, own_ref, *refs):
        part_refs, key_ref, value_ref = (refs[:-2], refs[-2], refs[-1])
        for column in range(count):
            keys = slice(column * 2 * DH, (column + 1) * 2 * DH)
            total = own_ref[:, keys]
            for part_ref in part_refs:
                total = total + part_ref[:, keys].astype(jnp.float32)
            head = pl.multiple_of((place_ref[0] ^ column) * DH, DH)
            key_ref[:, pl.ds(head, DH)] = total[:, :DH]
            value_ref[:, pl.ds(head, DH)] = total[:, DH:]

    shape = shaped((rows, count * DH), jnp.float32)
    return call(sum_parts, [shape] * 2, (place, own, *parts), 1)


def joined_queries(place, parts):
    count = len(parts)
    rows, width = parts[0].shape

    def join_queries(place_ref, *refs):
        for distance in range(count):
            first = pl.multiple_of((place_ref[0] ^ distance) * width, width)
            refs[-1][:, pl.ds(first, width)] = refs[distance][...]

    return call(join_queries, [shaped((rows, count * width))], (place, *parts), 1)[0]


def head_shards(hidden_in, queries, key_states, value_states, grad_out, log_sums, deltas, block_order):
    count = lax.axis_size("seq")
    owners = lax.axis_size("batch")
    my_index = lax.axis_index("seq").astype(jnp.int32)
    place = my_index.reshape(1)
    owner = lax.axis_index("batch").astype(jnp.int32).reshape(1)
    rows = queries.shape[1]
    group_size = HQ // HK
    peers = my_index ^ jnp.arange(count, dtype=jnp.int32)
    terms = jnp.concatenate(
        [log_sums.reshape(count, group_size, rows), deltas.reshape(count, group_size, rows)], axis=1
    )
    order = jnp.take(block_order.reshape(count, -1), peers, axis=0).reshape(-1)
    far_first = sorted(range(1, count), reverse=True)

    payloads = head_payloads(place, queries[0], grad_out[0], key_states[0], value_states[0], count)
    row_terms = [
        lax.dynamic_index_in_dim(terms, peers[distance], 0, keepdims=False)
        for distance in range(count)
    ]
    for distance in far_first:
        row_terms[distance] = swapped(row_terms[distance], "seq", distance)
        payloads[distance] = swapped(payloads[distance], "seq", distance)
    features = feature_payloads(place, hidden_in[0], count, owners)
    for distance in far_first:
        features[distance] = swapped(features[distance], "seq", distance)
    query_parts, tokens = head_grads(order, payloads, row_terms, rows * count // block_order.shape[0])
    step = count // 2
    held = {0: tokens}
    while step:
        for distance in list(held):
            held[distance ^ step] = swapped(held[distance], "seq", step)
        step //= 2
    all_tokens = [held[distance] for distance in range(count)]
    query_parts = list(query_parts)
    for distance in far_first:
        query_parts[distance] = swapped(query_parts[distance], "seq", distance)
    own, grad_keys, grad_values, parts = weight_parts((place, owner), features, all_tokens, owners)
    parts = [swapped(part, "batch", index + 1) for index, part in reversed(list(enumerate(parts)))]
    grad_queries = joined_queries(place, query_parts)
    key_wgrad, value_wgrad = summed_parts(place, own, parts, count)
    return (grad_queries[None], grad_keys[None], grad_values[None], key_wgrad, value_wgrad)


def shards(*args):
    count, owners = (lax.axis_size("seq"), lax.axis_size("batch"))
    own = args[0].shape[2] // (count * owners)
    fits = count == HK and owners & (owners - 1) == 0 and args[1].shape[0] == 1
    if fits and args[1].shape[1] % 128 == 0 and own % 16 == 0:
        return head_shards(*args)
    return ring_shards(*args)


def solution(mesh):
    in_specs = (
        P("batch", "seq", None),
        P("batch", "seq", None),
        P("batch", "seq", None),
        P("batch", "seq", None),
        P("batch", "seq", None),
        P("batch", None, "seq"),
        P("batch", None, "seq"),
        P(),
    )
    out_specs = (
        P("batch", "seq", None),
        P("batch", "seq", None),
        P("batch", "seq", None),
        P(("batch", "seq"), None),
        P(("batch", "seq"), None),
    )
    return jax.shard_map(shards, mesh=mesh, in_specs=in_specs, out_specs=out_specs, check_vma=False)
```

```python
import math

import jax
import jax.numpy as jnp
from jax import lax
from jax.experimental import pallas as pl
from jax.experimental.pallas import tpu as pltpu
from jax.sharding import PartitionSpec as P

HQ = 16
HK = 4
DH = 128


MASKED = -1e30


def passed_along(value, axis, steps):
    count = lax.axis_size(axis)
    pairs = [(source, (source + steps) % count) for source in range(count)]
    return lax.ppermute(value, axis, pairs)


def stored_positions(block_order, first_row, row_count, span_rows):
    row_ids = first_row + jnp.arange(row_count, dtype=jnp.int32)
    slot_ids = row_ids // span_rows
    matches = slot_ids[:, None] == jnp.arange(block_order.shape[0], dtype=jnp.int32)[None, :]
    block_ids = jnp.sum(jnp.where(matches, block_order[None, :], 0), axis=1)
    return block_ids * span_rows + row_ids % span_rows


def head_scores(left_heads, right_block):
    batch_rows, right_rows = (right_block.shape[0], right_block.shape[1])
    right_heads = right_block.reshape(batch_rows, right_rows, HK, DH)
    return jnp.einsum(
        "bqhgd,bkhd->bhgqk", left_heads, right_heads, preferred_element_type=jnp.float32
    )


def masked_scores(query_heads, key_block, query_pos, key_pos):
    scores = head_scores(query_heads, key_block) * (1.0 / math.sqrt(DH))
    visible = key_pos[None, :] <= query_pos[:, None]
    return jnp.where(visible, scores, MASKED)


def grad_block(
    query_heads, grad_heads, query_pos, row_lse, row_deltas, key_block, value_block, key_pos
):
    scores = masked_scores(query_heads, key_block, query_pos, key_pos)
    probs = jnp.exp(scores - row_lse[..., None])
    grad_probs = head_scores(grad_heads, value_block)
    grad_scores = (probs * (grad_probs - row_deltas[..., None]) * (1.0 / math.sqrt(DH))).astype(
        jnp.bfloat16
    )
    probs_low = probs.astype(jnp.bfloat16)
    batch_rows, key_rows = (key_block.shape[0], key_block.shape[1])
    key_heads = key_block.reshape(batch_rows, key_rows, HK, DH)
    query_part = jnp.einsum(
        "bhgqk,bkhd->bqhgd", grad_scores, key_heads, preferred_element_type=jnp.float32
    )
    key_part = jnp.einsum(
        "bhgqk,bqhgd->bkhd", grad_scores, query_heads, preferred_element_type=jnp.float32
    )
    value_part = jnp.einsum(
        "bhgqk,bqhgd->bkhd", probs_low, grad_heads, preferred_element_type=jnp.float32
    )
    key_part = key_part.reshape(batch_rows, key_rows, HK * DH)
    value_part = value_part.reshape(batch_rows, key_rows, HK * DH)
    return (query_part, key_part, value_part)


def ring_shards(hidden_in, queries, key_states, value_states, grad_out, log_sums, deltas, block_order):
    seq_count = lax.axis_size("seq")
    my_index = lax.axis_index("seq")
    batch_rows, local_rows = (queries.shape[0], queries.shape[1])
    span_rows = local_rows // 2
    group_size = HQ // HK
    query_heads = queries.reshape(batch_rows, local_rows, HK, group_size, DH)
    grad_heads = grad_out.reshape(batch_rows, local_rows, HK, group_size, DH)
    row_lse = log_sums.reshape(batch_rows, HK, group_size, local_rows)
    row_deltas = deltas.reshape(batch_rows, HK, group_size, local_rows)
    query_pos = stored_positions(block_order, my_index * local_rows, local_rows, span_rows)
    key_zeros = jnp.zeros(key_states.shape, jnp.float32)
    query_zeros = jnp.zeros(query_heads.shape, jnp.float32)

    def block_grads(accums, key_block, value_block, source):
        key_acc, value_acc, query_acc = accums
        key_pos = stored_positions(block_order, source * local_rows, local_rows, span_rows)
        query_part, key_part, value_part = grad_block(
            query_heads, grad_heads, query_pos, row_lse, row_deltas, key_block, value_block, key_pos
        )
        return (key_acc + key_part, value_acc + value_part, query_acc + query_part)

    whole_keys, whole_values = (
        lax.all_gather(key_states, "seq", axis=1, tiled=True),
        lax.all_gather(value_states, "seq", axis=1, tiled=True),
    )

    def back_turn(turn_index, accums):
        source = (my_index + turn_index + 1) % seq_count
        key_block = lax.dynamic_slice_in_dim(whole_keys, source * local_rows, local_rows, 1)
        value_block = lax.dynamic_slice_in_dim(whole_values, source * local_rows, local_rows, 1)
        return block_grads(accums, key_block, value_block, source)

    def back_step(turn_index, accums):
        key_acc, value_acc, query_acc = back_turn(turn_index, accums)
        key_acc, value_acc = passed_along((key_acc, value_acc), "seq", -1)
        return (key_acc, value_acc, query_acc)

    accums = lax.fori_loop(0, seq_count - 1, back_step, (key_zeros, key_zeros, query_zeros))
    key_acc, value_acc, query_acc = back_turn(seq_count - 1, accums)
    grad_keys = key_acc.astype(jnp.bfloat16)
    grad_values = value_acc.astype(jnp.bfloat16)
    grad_queries = query_acc.reshape(batch_rows, local_rows, HQ * DH).astype(jnp.bfloat16)
    key_width = HK * DH
    token_grads = jnp.concatenate([grad_keys, grad_values], axis=2).reshape(
        batch_rows * local_rows, 2 * key_width
    )
    flat_hidden = hidden_in.reshape(batch_rows * local_rows, hidden_in.shape[2])
    weight_grads = lax.psum_scatter(
        jnp.einsum("td,te->de", flat_hidden, token_grads, preferred_element_type=jnp.float32),
        ("batch", "seq"),
        scatter_dimension=0,
        tiled=True,
    )
    return (
        grad_queries,
        grad_keys,
        grad_values,
        weight_grads[:, :key_width],
        weight_grads[:, key_width:],
    )


def swapped(value, axis, distance):
    count = lax.axis_size(axis)
    return lax.ppermute(value, axis, [(source, source ^ distance) for source in range(count)])


def dot(left, right, left_dim, right_dim):
    dims = (((left_dim,), (right_dim,)), ((), ()))
    return lax.dot_general(left, right, dims, preferred_element_type=jnp.float32)


def vmem():
    return pl.BlockSpec(memory_space=pltpu.VMEM)


def smem():
    return pl.BlockSpec(memory_space=pltpu.SMEM)


def call(body, out_shapes, operands, scalars, scratch=(), after=()):
    specs = [smem()] * scalars + [vmem()] * (len(operands) - scalars)
    specs += [pl.BlockSpec(memory_space=pl.ANY)] * len(after)
    outs = pl.pallas_call(
        body,
        out_shape=out_shapes,
        in_specs=specs,
        out_specs=[vmem()] * len(out_shapes),
        scratch_shapes=scratch,
    )(*operands, *after)
    return list(outs)


def shaped(shape, dtype=jnp.bfloat16):
    return jax.ShapeDtypeStruct(shape, dtype)


def head_payloads(place, queries, grad_out, keys, values, log_sums, deltas, count):
    rows, query_width = queries.shape
    key_width = keys.shape[1]
    query_part, key_part = (query_width // count, key_width // count)
    heads = log_sums.shape[0]
    part = heads // count

    def pack_heads(place_ref, query_ref, grad_ref, key_ref, value_ref, lse_ref, delta_ref, *refs):
        out_refs, term_refs = (refs[:count], refs[count:])

        def own_heads(source_ref, peer):
            chosen = source_ref[:part, :]
            for index in range(1, count):
                chosen = jnp.where(
                    peer == index, source_ref[index * part : (index + 1) * part, :], chosen
                )
            return chosen

        for distance, out_ref in enumerate(out_refs):
            peer = place_ref[0] ^ distance
            wide = pl.ds(pl.multiple_of(peer * query_part, query_part), query_part)
            thin = pl.ds(pl.multiple_of(peer * key_part, key_part), key_part)
            out_ref[:, :query_part] = query_ref[:, wide]
            out_ref[:, query_part : 2 * query_part] = grad_ref[:, wide]
            out_ref[:, 2 * query_part : 2 * query_part + key_part] = key_ref[:, thin]
            out_ref[:, 2 * query_part + key_part :] = value_ref[:, thin]
            term_refs[distance][:part, :] = own_heads(lse_ref, peer)
            term_refs[distance][part:, :] = own_heads(delta_ref, peer)

    shapes = [shaped((rows, 2 * query_part + 2 * key_part))] * count
    shapes += [shaped((2 * part, rows), jnp.float32)] * count
    operands = (place, queries, grad_out, keys, values, log_sums, deltas)
    outs = call(pack_heads, shapes, operands, 1)
    return (outs[:count], outs[count:])


def feature_payloads(place, hidden, count, owners, after):
    rows, width = hidden.shape
    own = width // (count * owners)

    def pack_features(place_ref, hidden_ref, _, *refs):
        out_refs, turned_ref = (refs[:-1], refs[-1])
        turned_ref[...] = hidden_ref[...].T
        for distance, out_ref in enumerate(out_refs):
            peer = place_ref[0] ^ distance
            for owner in range(owners):
                first = pl.multiple_of((owner * count + peer) * own, own)
                out_ref[owner * own : (owner + 1) * own, :] = turned_ref[pl.ds(first, own), :]

    shape = shaped((owners * own, rows))
    scratch = [pltpu.VMEM((width, rows), jnp.bfloat16)]
    return call(pack_features, [shape] * count, (place, hidden), 1, scratch, (after,))


def head_grads(place, order, payloads, row_terms, span_rows, after):
    count = len(payloads)
    rows = payloads[0].shape[0]
    group_size = row_terms[0].shape[0] // 2
    total = count * rows
    spans = total // span_rows
    held = rows // span_rows
    tile = min(total, 256)
    query_part = group_size * DH

    def attention_grads(place_ref, order_ref, *refs):
        data_refs, term_refs = (refs[:count], refs[count : 2 * count])
        query_refs, token_ref = (refs[2 * count + 1 : 3 * count + 1], refs[3 * count + 1])

        def positions(shape, dim):
            ids = lax.broadcasted_iota(jnp.int32, shape, dim)
            result = ids % span_rows
            slots = ids // span_rows
            for span in range(spans):
                stored = (place_ref[0] ^ (span // held)) * held + span % held
                result = jnp.where(slots == span, result + order_ref[stored] * span_rows, result)
            return result

        def columns(first):
            return jnp.concatenate([ref[:, first : first + DH] for ref in data_refs], axis=0)

        query_pos = positions((1, total), 1)
        key_pos = positions((total, 1), 0)
        keys = columns(2 * query_part)
        values = columns(2 * query_part + DH)
        scale = 1.0 / math.sqrt(DH)
        hidden_add = [
            jnp.where(key_pos[first : first + tile] <= query_pos, 0.0, MASKED)
            for first in range(0, total, tile)
        ]
        key_sums = [None] * (total // tile)
        value_sums = [None] * (total // tile)
        for head in range(group_size):
            queries = columns(head * DH)
            grads = columns(query_part + head * DH)
            lse = jnp.concatenate([ref[head : head + 1, :] for ref in term_refs], axis=1)
            deltas = jnp.concatenate(
                [ref[group_size + head : group_size + head + 1, :] for ref in term_refs], axis=1
            )
            query_sum = None
            for index in range(total // tile):
                part = slice(index * tile, (index + 1) * tile)
                scores = dot(keys[part], queries, 1, 1) * scale + hidden_add[index]
                probs = jnp.exp(scores - lse)
                grad_probs = dot(values[part], grads, 1, 1)
                grad_scores = (probs * (grad_probs - deltas) * scale).astype(jnp.bfloat16)
                key_part = dot(grad_scores, queries, 1, 0)
                value_part = dot(probs.astype(jnp.bfloat16), grads, 1, 0)
                query_tile = dot(grad_scores, keys[part], 0, 0)
                query_sum = query_tile if index == 0 else query_sum + query_tile
                key_sums[index] = key_part if head == 0 else key_sums[index] + key_part
                value_sums[index] = value_part if head == 0 else value_sums[index] + value_part
            for source, out_ref in enumerate(query_refs):
                out_ref[:, head * DH : (head + 1) * DH] = query_sum[
                    source * rows : (source + 1) * rows
                ].astype(jnp.bfloat16)
        for index in range(total // tile):
            part = slice(index * tile, (index + 1) * tile)
            token_ref[part, :DH] = key_sums[index].astype(jnp.bfloat16)
            token_ref[part, DH:] = value_sums[index].astype(jnp.bfloat16)

    shapes = [shaped((rows, query_part))] * count + [shaped((total, 2 * DH))]
    outs = call(attention_grads, shapes, (place, order, *payloads, *row_terms), 2, (), (after,))
    return (outs[:count], outs[count])


def weight_parts(owner, features, tokens, owners):
    count = len(features)
    width, rows = features[0].shape
    own = width // owners
    shifts = [shift for shift, _ in tokens]

    def weight_grads(owner_ref, *refs):
        feature_refs, token_refs = (refs[:count], refs[count : count + len(shifts)])
        own_ref, part_refs, sum_ref = (refs[count + len(shifts)], refs[count + len(shifts) + 1 : -1], refs[-1])
        left = jnp.concatenate([ref[...] for ref in feature_refs], axis=1)
        for column, (shift, token_ref) in enumerate(zip(shifts, token_refs)):
            right = jnp.concatenate(
                [
                    token_ref[(shift ^ source) * rows : ((shift ^ source) + 1) * rows, :]
                    for source in range(count)
                ],
                axis=0,
            )
            sum_ref[:, column * 2 * DH : (column + 1) * 2 * DH] = dot(left, right, 1, 0)
        first = pl.multiple_of(owner_ref[0] * own, own)
        own_ref[...] = sum_ref[pl.ds(first, own), :]
        for index, part_ref in enumerate(part_refs):
            first = pl.multiple_of((owner_ref[0] ^ (index + 1)) * own, own)
            part_ref[...] = sum_ref[pl.ds(first, own), :].astype(jnp.bfloat16)

    columns = len(shifts) * 2 * DH
    shapes = [shaped((own, columns), jnp.float32)] + [shaped((own, columns))] * (owners - 1)
    scratch = [pltpu.VMEM((width, columns), jnp.float32)]
    operands = (owner, *features, *[held for _, held in tokens])
    outs = call(weight_grads, shapes, operands, 1, scratch)
    return (outs[0], outs[1:])


def summed(own, parts):
    def sum_parts(own_ref, *refs):
        total = own_ref[...]
        for part_ref in refs[:-1]:
            total = total + part_ref[...].astype(jnp.float32)
        refs[-1][...] = total

    return call(sum_parts, [shaped(own.shape, jnp.float32)], (own, *parts), 0)[0]


def summed_last(place, done, own, parts, count):
    rows, width = own.shape

    def sum_last_parts(place_ref, *refs):
        done_refs, own_ref = (refs[: len(done)], refs[len(done)])
        part_refs, key_ref, value_ref = (refs[len(done) + 1 : -2], refs[-2], refs[-1])
        last = own_ref[...]
        for part_ref in part_refs:
            last = last + part_ref[...].astype(jnp.float32)
        pieces = [ref[...] for ref in done_refs] + [last]
        for index, piece in enumerate(pieces):
            for column in range(width // (2 * DH)):
                shift = index * (width // (2 * DH)) + column
                head = pl.multiple_of((place_ref[0] ^ shift) * DH, DH)
                first = column * 2 * DH
                key_ref[:, pl.ds(head, DH)] = piece[:, first : first + DH]
                value_ref[:, pl.ds(head, DH)] = piece[:, first + DH : first + 2 * DH]

    shape = shaped((rows, count * DH), jnp.float32)
    return call(sum_last_parts, [shape] * 2, (place, *done, own, *parts), 1)


def joined_rows(place, query_parts, tokens):
    count = len(query_parts)
    rows, width = query_parts[0].shape

    def join_rows(place_ref, *refs):
        part_refs, token_refs = (refs[:count], refs[count : 2 * count])
        query_ref, key_ref, value_ref = refs[2 * count :]
        for distance in range(count):
            peer = place_ref[0] ^ distance
            wide = pl.ds(pl.multiple_of(peer * width, width), width)
            thin = pl.ds(pl.multiple_of(peer * DH, DH), DH)
            mine = slice(distance * rows, (distance + 1) * rows)
            query_ref[:, wide] = part_refs[distance][...]
            key_ref[:, thin] = token_refs[distance][mine, :DH]
            value_ref[:, thin] = token_refs[distance][mine, DH:]

    shapes = [shaped((rows, count * width))] + [shaped((rows, count * DH))] * 2
    return call(join_rows, shapes, (place, *query_parts, *tokens), 1)


def head_shards(hidden_in, queries, key_states, value_states, grad_out, log_sums, deltas, block_order):
    count = lax.axis_size("seq")
    owners = lax.axis_size("batch")
    place = lax.axis_index("seq").astype(jnp.int32).reshape(1)
    owner = lax.axis_index("batch").astype(jnp.int32).reshape(1)
    span_rows = queries.shape[1] * count // block_order.shape[0]
    far_first = sorted(range(1, count), reverse=True)

    payloads, row_terms = head_payloads(
        place, queries[0], grad_out[0], key_states[0], value_states[0], log_sums[0], deltas[0], count
    )
    features = feature_payloads(place, hidden_in[0], count, owners, payloads[0])
    local_features = features[0]
    for distance in far_first:
        row_terms[distance] = swapped(row_terms[distance], "seq", distance)
        payloads[distance] = swapped(payloads[distance], "seq", distance)
    for distance in far_first:
        features[distance] = swapped(features[distance], "seq", distance)
    query_parts, tokens = head_grads(
        place, block_order, payloads, row_terms, span_rows, local_features
    )
    held = {0: tokens}
    half = count // 2
    held[half] = swapped(tokens, "seq", half)
    step = half // 2
    while step:
        for distance in sorted(held):
            held[distance ^ step] = swapped(held[distance], "seq", step)
        step //= 2
    done = []
    for group in range(2):
        some = [(shift, held[shift]) for shift in range(group * half, (group + 1) * half)]
        own, parts = weight_parts(owner, features, some, owners)
        parts = [
            swapped(part, "batch", index + 1)
            for index, part in reversed(list(enumerate(parts)))
        ]
        if group == 0:
            done.append(summed(own, parts))
    for distance in far_first:
        query_parts[distance] = swapped(query_parts[distance], "seq", distance)
    all_tokens = [held[distance] for distance in range(count)]
    grad_queries, grad_keys, grad_values = joined_rows(place, query_parts, all_tokens)
    key_wgrad, value_wgrad = summed_last(place, done, own, parts, count)
    return (grad_queries[None], grad_keys[None], grad_values[None], key_wgrad, value_wgrad)


def shards(*args):
    count, owners = (lax.axis_size("seq"), lax.axis_size("batch"))
    own = args[0].shape[2] // (count * owners)
    fits = count == HK and owners & (owners - 1) == 0 and args[1].shape[0] == 1
    if fits and args[1].shape[1] % 128 == 0 and own % 16 == 0:
        return head_shards(*args)
    return ring_shards(*args)


def solution(mesh):
    in_specs = (
        P("batch", "seq", None),
        P("batch", "seq", None),
        P("batch", "seq", None),
        P("batch", "seq", None),
        P("batch", "seq", None),
        P("batch", None, "seq"),
        P("batch", None, "seq"),
        P(),
    )
    out_specs = (
        P("batch", "seq", None),
        P("batch", "seq", None),
        P("batch", "seq", None),
        P(("batch", "seq"), None),
        P(("batch", "seq"), None),
    )
    return jax.shard_map(shards, mesh=mesh, in_specs=in_specs, out_specs=out_specs, check_vma=False)
```

```python
import math

import jax
import jax.numpy as jnp
from jax import lax
from jax.experimental import pallas as pl
from jax.experimental.pallas import tpu as pltpu
from jax.sharding import PartitionSpec as P

HQ = 16
HK = 4
DH = 128


MASKED = -1e30


def passed_along(value, axis, steps):
    count = lax.axis_size(axis)
    pairs = [(source, (source + steps) % count) for source in range(count)]
    return lax.ppermute(value, axis, pairs)


def stored_positions(block_order, first_row, row_count, span_rows):
    row_ids = first_row + jnp.arange(row_count, dtype=jnp.int32)
    slot_ids = row_ids // span_rows
    matches = slot_ids[:, None] == jnp.arange(block_order.shape[0], dtype=jnp.int32)[None, :]
    block_ids = jnp.sum(jnp.where(matches, block_order[None, :], 0), axis=1)
    return block_ids * span_rows + row_ids % span_rows


def head_scores(left_heads, right_block):
    batch_rows, right_rows = (right_block.shape[0], right_block.shape[1])
    right_heads = right_block.reshape(batch_rows, right_rows, HK, DH)
    return jnp.einsum(
        "bqhgd,bkhd->bhgqk", left_heads, right_heads, preferred_element_type=jnp.float32
    )


def masked_scores(query_heads, key_block, query_pos, key_pos):
    scores = head_scores(query_heads, key_block) * (1.0 / math.sqrt(DH))
    visible = key_pos[None, :] <= query_pos[:, None]
    return jnp.where(visible, scores, MASKED)


def grad_block(
    query_heads, grad_heads, query_pos, row_lse, row_deltas, key_block, value_block, key_pos
):
    scores = masked_scores(query_heads, key_block, query_pos, key_pos)
    probs = jnp.exp(scores - row_lse[..., None])
    grad_probs = head_scores(grad_heads, value_block)
    grad_scores = (probs * (grad_probs - row_deltas[..., None]) * (1.0 / math.sqrt(DH))).astype(
        jnp.bfloat16
    )
    probs_low = probs.astype(jnp.bfloat16)
    batch_rows, key_rows = (key_block.shape[0], key_block.shape[1])
    key_heads = key_block.reshape(batch_rows, key_rows, HK, DH)
    query_part = jnp.einsum(
        "bhgqk,bkhd->bqhgd", grad_scores, key_heads, preferred_element_type=jnp.float32
    )
    key_part = jnp.einsum(
        "bhgqk,bqhgd->bkhd", grad_scores, query_heads, preferred_element_type=jnp.float32
    )
    value_part = jnp.einsum(
        "bhgqk,bqhgd->bkhd", probs_low, grad_heads, preferred_element_type=jnp.float32
    )
    key_part = key_part.reshape(batch_rows, key_rows, HK * DH)
    value_part = value_part.reshape(batch_rows, key_rows, HK * DH)
    return (query_part, key_part, value_part)


def ring_shards(hidden_in, queries, key_states, value_states, grad_out, log_sums, deltas, block_order):
    seq_count = lax.axis_size("seq")
    my_index = lax.axis_index("seq")
    batch_rows, local_rows = (queries.shape[0], queries.shape[1])
    span_rows = local_rows // 2
    group_size = HQ // HK
    query_heads = queries.reshape(batch_rows, local_rows, HK, group_size, DH)
    grad_heads = grad_out.reshape(batch_rows, local_rows, HK, group_size, DH)
    row_lse = log_sums.reshape(batch_rows, HK, group_size, local_rows)
    row_deltas = deltas.reshape(batch_rows, HK, group_size, local_rows)
    query_pos = stored_positions(block_order, my_index * local_rows, local_rows, span_rows)
    key_zeros = jnp.zeros(key_states.shape, jnp.float32)
    query_zeros = jnp.zeros(query_heads.shape, jnp.float32)

    def block_grads(accums, key_block, value_block, source):
        key_acc, value_acc, query_acc = accums
        key_pos = stored_positions(block_order, source * local_rows, local_rows, span_rows)
        query_part, key_part, value_part = grad_block(
            query_heads, grad_heads, query_pos, row_lse, row_deltas, key_block, value_block, key_pos
        )
        return (key_acc + key_part, value_acc + value_part, query_acc + query_part)

    whole_keys, whole_values = (
        lax.all_gather(key_states, "seq", axis=1, tiled=True),
        lax.all_gather(value_states, "seq", axis=1, tiled=True),
    )

    def back_turn(turn_index, accums):
        source = (my_index + turn_index + 1) % seq_count
        key_block = lax.dynamic_slice_in_dim(whole_keys, source * local_rows, local_rows, 1)
        value_block = lax.dynamic_slice_in_dim(whole_values, source * local_rows, local_rows, 1)
        return block_grads(accums, key_block, value_block, source)

    def back_step(turn_index, accums):
        key_acc, value_acc, query_acc = back_turn(turn_index, accums)
        key_acc, value_acc = passed_along((key_acc, value_acc), "seq", -1)
        return (key_acc, value_acc, query_acc)

    accums = lax.fori_loop(0, seq_count - 1, back_step, (key_zeros, key_zeros, query_zeros))
    key_acc, value_acc, query_acc = back_turn(seq_count - 1, accums)
    grad_keys = key_acc.astype(jnp.bfloat16)
    grad_values = value_acc.astype(jnp.bfloat16)
    grad_queries = query_acc.reshape(batch_rows, local_rows, HQ * DH).astype(jnp.bfloat16)
    key_width = HK * DH
    token_grads = jnp.concatenate([grad_keys, grad_values], axis=2).reshape(
        batch_rows * local_rows, 2 * key_width
    )
    flat_hidden = hidden_in.reshape(batch_rows * local_rows, hidden_in.shape[2])
    weight_grads = lax.psum_scatter(
        jnp.einsum("td,te->de", flat_hidden, token_grads, preferred_element_type=jnp.float32),
        ("batch", "seq"),
        scatter_dimension=0,
        tiled=True,
    )
    return (
        grad_queries,
        grad_keys,
        grad_values,
        weight_grads[:, :key_width],
        weight_grads[:, key_width:],
    )


def swapped(value, axis, distance):
    count = lax.axis_size(axis)
    return lax.ppermute(value, axis, [(source, source ^ distance) for source in range(count)])


def dot(left, right, left_dim, right_dim):
    dims = (((left_dim,), (right_dim,)), ((), ()))
    return lax.dot_general(left, right, dims, preferred_element_type=jnp.float32)


def vmem():
    return pl.BlockSpec(memory_space=pltpu.VMEM)


def smem():
    return pl.BlockSpec(memory_space=pltpu.SMEM)


def call(body, out_shapes, operands, scalars, scratch=(), after=()):
    specs = [smem()] * scalars + [vmem()] * (len(operands) - scalars)
    specs += [pl.BlockSpec(memory_space=pl.ANY)] * len(after)
    outs = pl.pallas_call(
        body,
        out_shape=out_shapes,
        in_specs=specs,
        out_specs=[vmem()] * len(out_shapes),
        scratch_shapes=scratch,
    )(*operands, *after)
    return list(outs)


def shaped(shape, dtype=jnp.bfloat16):
    return jax.ShapeDtypeStruct(shape, dtype)


def head_payloads(place, queries, grad_out, keys, values, log_sums, deltas, count):
    rows, query_width = queries.shape
    key_width = keys.shape[1]
    query_part, key_part = (query_width // count, key_width // count)
    heads = log_sums.shape[0]
    part = heads // count

    def pack_heads(place_ref, query_ref, grad_ref, key_ref, value_ref, lse_ref, delta_ref, *refs):
        out_refs, term_refs = (refs[:count], refs[count:])

        def own_heads(source_ref, peer):
            chosen = source_ref[:part, :]
            for index in range(1, count):
                chosen = jnp.where(
                    peer == index, source_ref[index * part : (index + 1) * part, :], chosen
                )
            return chosen

        for distance, out_ref in enumerate(out_refs):
            peer = place_ref[0] ^ distance
            wide = pl.ds(pl.multiple_of(peer * query_part, query_part), query_part)
            thin = pl.ds(pl.multiple_of(peer * key_part, key_part), key_part)
            out_ref[:, :query_part] = query_ref[:, wide]
            out_ref[:, query_part : 2 * query_part] = grad_ref[:, wide]
            out_ref[:, 2 * query_part : 2 * query_part + key_part] = key_ref[:, thin]
            out_ref[:, 2 * query_part + key_part :] = value_ref[:, thin]
            term_refs[distance][:part, :] = own_heads(lse_ref, peer)
            term_refs[distance][part:, :] = own_heads(delta_ref, peer)

    shapes = [shaped((rows, 2 * query_part + 2 * key_part))] * count
    shapes += [shaped((2 * part, rows), jnp.float32)] * count
    operands = (place, queries, grad_out, keys, values, log_sums, deltas)
    outs = call(pack_heads, shapes, operands, 1)
    return (outs[:count], outs[count:])


def feature_payloads(place, hidden, count, owners, after):
    rows, width = hidden.shape
    own = width // (count * owners)

    def pack_features(place_ref, hidden_ref, _, *refs):
        out_refs, turned_ref = (refs[:-1], refs[-1])
        turned_ref[...] = hidden_ref[...].T
        for distance, out_ref in enumerate(out_refs):
            peer = place_ref[0] ^ distance
            for owner in range(owners):
                first = pl.multiple_of((owner * count + peer) * own, own)
                out_ref[owner * own : (owner + 1) * own, :] = turned_ref[pl.ds(first, own), :]

    shape = shaped((owners * own, rows))
    scratch = [pltpu.VMEM((width, rows), jnp.bfloat16)]
    return call(pack_features, [shape] * count, (place, hidden), 1, scratch, (after,))


def head_grads(place, order, payloads, row_terms, span_rows, after):
    count = len(payloads)
    rows = payloads[0].shape[0]
    group_size = row_terms[0].shape[0] // 2
    total = count * rows
    spans = total // span_rows
    held = rows // span_rows
    tile = min(total, 256)
    query_part = group_size * DH

    def attention_grads(place_ref, order_ref, *refs):
        data_refs, term_refs = (refs[:count], refs[count : 2 * count])
        query_refs, token_ref = (refs[2 * count + 1 : 3 * count + 1], refs[3 * count + 1])

        def positions(shape, dim):
            ids = lax.broadcasted_iota(jnp.int32, shape, dim)
            result = ids % span_rows
            slots = ids // span_rows
            for span in range(spans):
                stored = (place_ref[0] ^ (span // held)) * held + span % held
                result = jnp.where(slots == span, result + order_ref[stored] * span_rows, result)
            return result

        def columns(first):
            return jnp.concatenate([ref[:, first : first + DH] for ref in data_refs], axis=0)

        query_pos = positions((1, total), 1)
        key_pos = positions((total, 1), 0)
        keys = columns(2 * query_part)
        values = columns(2 * query_part + DH)
        scale = 1.0 / math.sqrt(DH)
        hidden_add = [
            jnp.where(key_pos[first : first + tile] <= query_pos, 0.0, MASKED)
            for first in range(0, total, tile)
        ]
        key_sums = [None] * (total // tile)
        value_sums = [None] * (total // tile)
        for head in range(group_size):
            queries = columns(head * DH)
            grads = columns(query_part + head * DH)
            lse = jnp.concatenate([ref[head : head + 1, :] for ref in term_refs], axis=1)
            deltas = jnp.concatenate(
                [ref[group_size + head : group_size + head + 1, :] for ref in term_refs], axis=1
            )
            query_sum = None
            for index in range(total // tile):
                part = slice(index * tile, (index + 1) * tile)
                scores = dot(keys[part], queries, 1, 1) * scale + hidden_add[index]
                probs = jnp.exp(scores - lse)
                grad_probs = dot(values[part], grads, 1, 1)
                grad_scores = (probs * (grad_probs - deltas) * scale).astype(jnp.bfloat16)
                key_part = dot(grad_scores, queries, 1, 0)
                value_part = dot(probs.astype(jnp.bfloat16), grads, 1, 0)
                query_tile = dot(grad_scores, keys[part], 0, 0)
                query_sum = query_tile if index == 0 else query_sum + query_tile
                key_sums[index] = key_part if head == 0 else key_sums[index] + key_part
                value_sums[index] = value_part if head == 0 else value_sums[index] + value_part
            for source, out_ref in enumerate(query_refs):
                out_ref[:, head * DH : (head + 1) * DH] = query_sum[
                    source * rows : (source + 1) * rows
                ].astype(jnp.bfloat16)
        for index in range(total // tile):
            part = slice(index * tile, (index + 1) * tile)
            token_ref[part, :DH] = key_sums[index].astype(jnp.bfloat16)
            token_ref[part, DH:] = value_sums[index].astype(jnp.bfloat16)

    shapes = [shaped((rows, query_part))] * count + [shaped((total, 2 * DH))]
    outs = call(attention_grads, shapes, (place, order, *payloads, *row_terms), 2, (), (after,))
    return (outs[:count], outs[count])


def weight_parts(owner, features, tokens, owners):
    count = len(features)
    width, rows = features[0].shape
    own = width // owners
    shifts = [shift for shift, _ in tokens]

    def weight_grads(owner_ref, *refs):
        feature_refs, token_refs = (refs[:count], refs[count : count + len(shifts)])
        own_ref, part_refs, sum_ref = (refs[count + len(shifts)], refs[count + len(shifts) + 1 : -1], refs[-1])
        left = jnp.concatenate([ref[...] for ref in feature_refs], axis=1)
        for column, (shift, token_ref) in enumerate(zip(shifts, token_refs)):
            right = jnp.concatenate(
                [
                    token_ref[(shift ^ source) * rows : ((shift ^ source) + 1) * rows, :]
                    for source in range(count)
                ],
                axis=0,
            )
            sum_ref[:, column * 2 * DH : (column + 1) * 2 * DH] = dot(left, right, 1, 0)
        first = pl.multiple_of(owner_ref[0] * own, own)
        own_ref[...] = sum_ref[pl.ds(first, own), :]
        for index, part_ref in enumerate(part_refs):
            first = pl.multiple_of((owner_ref[0] ^ (index + 1)) * own, own)
            part_ref[...] = sum_ref[pl.ds(first, own), :].astype(jnp.bfloat16)

    columns = len(shifts) * 2 * DH
    shapes = [shaped((own, columns), jnp.float32)] + [shaped((own, columns))] * (owners - 1)
    scratch = [pltpu.VMEM((width, columns), jnp.float32)]
    operands = (owner, *features, *[held for _, held in tokens])
    outs = call(weight_grads, shapes, operands, 1, scratch)
    return (outs[0], outs[1:])


def finished(place, groups, query_parts, tokens):
    count = len(query_parts)
    rows, query_width = query_parts[0].shape
    own_rows, width = groups[0][0].shape
    sizes = [1 + len(parts) for _, parts in groups]
    heads = width // (2 * DH)

    def finish(place_ref, *refs):
        query_ref, key_ref, value_ref, key_sum_ref, value_sum_ref = refs[-5:]
        first_ref = 0
        for index, size in enumerate(sizes):
            group_refs = refs[first_ref : first_ref + size]
            first_ref += size
            for column in range(heads):
                head = pl.multiple_of((place_ref[0] ^ (index * heads + column)) * DH, DH)
                for offset, out_ref in enumerate((key_sum_ref, value_sum_ref)):
                    part = pl.ds((2 * column + offset) * DH, DH)
                    total = group_refs[0][:, part]
                    for part_ref in group_refs[1:]:
                        total = total + part_ref[:, part].astype(jnp.float32)
                    out_ref[:, pl.ds(head, DH)] = total
        part_refs = refs[first_ref : first_ref + count]
        token_refs = refs[first_ref + count : first_ref + 2 * count]
        for distance in range(count):
            peer = place_ref[0] ^ distance
            wide = pl.ds(pl.multiple_of(peer * query_width, query_width), query_width)
            thin = pl.ds(pl.multiple_of(peer * DH, DH), DH)
            query_ref[:, wide] = part_refs[distance][...]
            key_ref[:, thin] = token_refs[distance][:, :DH]
            value_ref[:, thin] = token_refs[distance][:, DH:]

    operands = [place]
    for own, parts in groups:
        operands += [own, *parts]
    operands += [*query_parts, *tokens]
    specs = [smem()]
    specs += [pl.BlockSpec(held.shape, lambda step: (0, 0)) for held in operands[1:-count]]
    specs += [
        pl.BlockSpec((rows, 2 * DH), lambda step, index=index: (index, 0)) for index in range(count)
    ]
    shapes = [shaped((rows, count * query_width))] + [shaped((rows, count * DH))] * 2
    shapes += [shaped((own_rows, count * DH), jnp.float32)] * 2
    return pl.pallas_call(
        finish,
        grid=(1,),
        out_shape=shapes,
        in_specs=specs,
        out_specs=[pl.BlockSpec(shape.shape, lambda step: (0, 0)) for shape in shapes],
        name="finish",
    )(*operands)


def head_shards(hidden_in, queries, key_states, value_states, grad_out, log_sums, deltas, block_order):
    count = lax.axis_size("seq")
    owners = lax.axis_size("batch")
    place = lax.axis_index("seq").astype(jnp.int32).reshape(1)
    owner = lax.axis_index("batch").astype(jnp.int32).reshape(1)
    span_rows = queries.shape[1] * count // block_order.shape[0]
    far_first = sorted(range(1, count), reverse=True)

    payloads, row_terms = head_payloads(
        place, queries[0], grad_out[0], key_states[0], value_states[0], log_sums[0], deltas[0], count
    )
    features = feature_payloads(place, hidden_in[0], count, owners, payloads[0])
    local_features = features[0]
    for distance in far_first:
        row_terms[distance] = swapped(row_terms[distance], "seq", distance)
        payloads[distance] = swapped(payloads[distance], "seq", distance)
    for distance in far_first:
        features[distance] = swapped(features[distance], "seq", distance)
    query_parts, tokens = head_grads(
        place, block_order, payloads, row_terms, span_rows, local_features
    )
    held = {0: tokens}
    half = count // 2
    held[half] = swapped(tokens, "seq", half)
    step = half // 2
    while step:
        for distance in sorted(held):
            held[distance ^ step] = swapped(held[distance], "seq", step)
        step //= 2
    groups = []
    for group in range(2):
        some = [(shift, held[shift]) for shift in range(group * half, (group + 1) * half)]
        own, parts = weight_parts(owner, features, some, owners)
        parts = [
            swapped(part, "batch", index + 1)
            for index, part in reversed(list(enumerate(parts)))
        ]
        groups.append((own, parts))
    for distance in far_first:
        query_parts[distance] = swapped(query_parts[distance], "seq", distance)
    all_tokens = [held[distance] for distance in range(count)]
    grad_queries, grad_keys, grad_values, key_wgrad, value_wgrad = finished(
        place, groups, query_parts, all_tokens
    )
    return (grad_queries[None], grad_keys[None], grad_values[None], key_wgrad, value_wgrad)


def shards(*args):
    count, owners = (lax.axis_size("seq"), lax.axis_size("batch"))
    own = args[0].shape[2] // (count * owners)
    fits = count == HK and owners & (owners - 1) == 0 and args[1].shape[0] == 1
    if fits and args[1].shape[1] % 128 == 0 and own % 16 == 0:
        return head_shards(*args)
    return ring_shards(*args)


def solution(mesh):
    in_specs = (
        P("batch", "seq", None),
        P("batch", "seq", None),
        P("batch", "seq", None),
        P("batch", "seq", None),
        P("batch", "seq", None),
        P("batch", None, "seq"),
        P("batch", None, "seq"),
        P(),
    )
    out_specs = (
        P("batch", "seq", None),
        P("batch", "seq", None),
        P("batch", "seq", None),
        P(("batch", "seq"), None),
        P(("batch", "seq"), None),
    )
    return jax.shard_map(shards, mesh=mesh, in_specs=in_specs, out_specs=out_specs, check_vma=False)
```
